256 devices in a mesh: stream: 64 (over x, z, y_hi), span: 4 (over y_lo, core).
Axes of the slice: x: 4, y: 4 (y_hi: 2, y_lo: 2; y = y_hi * 2 + y_lo), z: 8, core: 2. Of those that a mesh axis runs over, the one named last changes fastest.
Arguments:
- state: float32 [2560, 8, 625], P('stream', 'span'), may hold values from -0.25 to 2.5, as said below
- direction: float32 [2560, 8, 625], P('stream', 'span'), may hold values from -6 to 6
- metric: float32 [2560, 8, 3], P('stream', 'span'), may hold values from 1 to 4
- face_source: int32 [2560, 4], P('stream'), may hold values from -1 to 225, as said below
- send_rows: int32 [64, 2, 33], P('stream'), may hold values from 0 to 159, as said below
Outputs:
- residual: float32 [2560, 8, 625], P('stream', 'span')
- basis_next: float32 [2560, 8, 625], P('stream', 'span')
- krylov: float32 [3], replicated
The draws below stay inside these ranges and needn't reach their ends.
Inputs may be any that keep to these rules, and one draw needn't show every extreme that they name: `state`: conserved variables from density 0.75 to 1.25, flow-wise velocity 0.1 to 0.5, other velocities -0.2 to 0.2, pressure 0.5 to 0.9, so pressure and temperature are positive. `face_source`: the plane is a grid of columns of 32 cells, numbered column by column, partition d owning cells d * 40 to (d + 1) * 40 - 1 in a random local order; flow-wise faces wrap around. Every face neighbour lies in the same or an adjacent partition; -1 stands exactly on the lower face of the lowest and the upper face of the highest row; indices into received blocks point at used slots. `send_rows`: at most 33 faces per neighbouring pair, and some pair uses all 33; slots beyond a pair's count hold 0; the order of slots is the order in which the receiver's face_source refers to them.
All inputs are finite; a program needn't handle non-finite values.
Results may differ from the reference program's by a relative error of at most 0.0003.
Values sent between devices are 32-bit elements.
No kernel may reach another device: no remote copies, remote signals or barrier semaphores. Data moves between devices by JAX's collectives and lax.ppermute only.
A program may use at most 128 MiB of HBM per device.

```python
import math
import jax
import jax.numpy as jnp
import numpy as np
from jax import lax

COLUMNS = 40
WALL_ROWS = 32
NODES = 125
VARS = 5
SLOTS = 33
PLANE = 2560
LAYERS = 8
N_STREAM = 64


GAMMA_RATIO = 1.4


def draw_state(key, part):
    noise_shape = (PLANE, LAYERS, 5, NODES)
    noise = jnp.clip(0.4 * jax.random.normal(key, noise_shape, jnp.float32), -1.0, 1.0)
    density = 1.0 + 0.25 * noise[:, :, 0]
    flow_speed = 0.3 + 0.2 * noise[:, :, 1]
    normal_speed = 0.2 * noise[:, :, 2]
    span_speed = 0.2 * noise[:, :, 3]
    pressure = 0.7 + 0.2 * noise[:, :, 4]
    kinetic = 0.5 * density * (flow_speed * flow_speed + normal_speed * normal_speed + span_speed * span_speed)
    energy = pressure / (GAMMA_RATIO - 1.0) + kinetic
    stacked = jnp.stack([density, density * flow_speed, density * normal_speed, density * span_speed, energy], axis=2)
    return stacked.reshape(PLANE, LAYERS, 5 * NODES)


def mesh_tables(key):
    devices = N_STREAM
    cell_ids = jnp.arange(PLANE, dtype=jnp.int32)
    owner_part = cell_ids // COLUMNS
    position = cell_ids % COLUMNS
    part_keys = jax.random.split(jax.random.fold_in(key, 17), devices)
    orders = jax.vmap(lambda single: jax.random.permutation(single, COLUMNS))(part_keys).astype(jnp.int32)
    local_column = orders[owner_part, position]
    column_count = PLANE // WALL_ROWS
    flow_column = cell_ids // WALL_ROWS
    wall_row = cell_ids % WALL_ROWS
    neighbor = jnp.stack([(flow_column - 1) % column_count * WALL_ROWS + wall_row, (flow_column + 1) % column_count * WALL_ROWS + wall_row, cell_ids - 1, cell_ids + 1], axis=1)
    walled = jnp.stack([wall_row < 0, wall_row < 0, wall_row == 0, wall_row == WALL_ROWS - 1], axis=1)
    neighbor = jnp.where(walled, cell_ids[:, None], neighbor)
    other_owner = neighbor // COLUMNS
    face_ids = jnp.arange(4, dtype=jnp.int32)[None, :]
    to_left = jnp.logical_and(jnp.logical_not(walled), other_owner == (owner_part[:, None] - 1) % devices)
    to_right = jnp.logical_and(jnp.logical_not(walled), other_owner == (owner_part[:, None] + 1) % devices)

    def slots_of(flags):
        flat_flags = flags.reshape(devices, COLUMNS * 4).astype(jnp.int32)
        before = jnp.cumsum(flat_flags, axis=1) - flat_flags
        return before.reshape(PLANE, 4)
    left_slot = slots_of(to_left)
    right_slot = slots_of(to_right)
    own_index = local_column[:, None] * 4 + face_ids
    owners = jnp.broadcast_to(owner_part[:, None], (PLANE, 4))
    send_table = jnp.zeros((devices, 2, SLOTS), jnp.int32)
    send_table = send_table.at[owners, 0, jnp.where(to_left, left_slot, SLOTS)].set(own_index, mode='drop')
    send_table = send_table.at[owners, 1, jnp.where(to_right, right_slot, SLOTS)].set(own_index, mode='drop')
    partner_face = face_ids + 1 - 2 * (face_ids % 2)
    partner_local = local_column[neighbor] * 4 + partner_face
    from_right = COLUMNS * 4 + SLOTS + left_slot[neighbor, partner_face]
    from_left = COLUMNS * 4 + right_slot[neighbor, partner_face]
    source = jnp.where(to_right, from_right, jnp.where(to_left, from_left, partner_local))
    source = jnp.where(walled, -1, source).astype(jnp.int32)
    row_ids = owner_part * COLUMNS + local_column
    source_table = jnp.zeros((PLANE, 4), jnp.int32).at[row_ids].set(source)
    return (source_table, send_table)


def draw_face_source(key, part):
    return mesh_tables(key)[0]


def draw_send_rows(key, part):
    return mesh_tables(key)[1]


def levels(key, shape, pieces, least, high):
    factor_of, own = 1.0, jax.random.fold_in(key, 6)
    for axis_at, shards_of in pieces:
        draws = jnp.exp(jax.random.uniform(jax.random.fold_in(own, axis_at), (shards_of,), jnp.float32, least / len(pieces), high / len(pieces)))
        factor_of = factor_of * jnp.repeat(draws, shape[axis_at] // shards_of).reshape([-1 if axis == axis_at else 1 for axis in range(len(shape))])
    return factor_of


def bell_draw(key, extent, scale, limit, shards=(), held_as=jnp.bfloat16):
    values = scale * jax.random.normal(key, extent, jnp.float32)
    if shards:
        values = values * levels(key, extent, shards, -0.22, 0.18)
    return jnp.clip(values, -limit, limit).astype(held_as)


def setup_inputs(seed: int = 0) -> dict:
    arg_keys = jax.random.split(jax.random.key(seed), 6)
    return {
        "state": draw_state(jax.random.fold_in(arg_keys[5], 71), 0),
        "direction": bell_draw(arg_keys[1], (PLANE, LAYERS, NODES * VARS), 1.0, 6.0, ((0, 64), (1, 4)), jnp.float32),
        "metric": jnp.clip(jnp.exp(math.log(4.0) - 1.3862944 * jax.random.uniform(arg_keys[2], (PLANE, LAYERS, 3), jnp.float32) ** levels(arg_keys[2], (PLANE, LAYERS, 3), ((0, 64), (1, 4)), -0.2, 0.2)), 1.0, 4.0),
        "face_source": draw_face_source(jax.random.fold_in(arg_keys[5], 71), 0),
        "send_rows": draw_send_rows(jax.random.fold_in(arg_keys[5], 71), 0),
    }


GAMMA = 1.4
VISC = 0.01
COND = VISC * GAMMA / ((GAMMA - 1.0) * 0.72)
LIFT = 10.0
EINSUM_FORMS = ('ai,...ijk->...ajk', 'aj,...ijk->...iak', 'ak,...ijk->...ija')

def diff_table():
    spread = math.sqrt(3.0 / 7.0)
    points = np.array([-1.0, -spread, 0.0, spread, 1.0])
    weights = np.array([np.prod([points[row_at] - points[other] for other in range(5) if other != row_at]) for row_at in range(5)])
    matrix = np.zeros((5, 5))
    for row_at in range(5):
        for col_at in range(5):
            if row_at != col_at:
                matrix[row_at, col_at] = weights[row_at] / (weights[col_at] * (points[row_at] - points[col_at]))
        matrix[row_at, row_at] = np.sum([1.0 / (points[row_at] - points[other]) for other in range(5) if other != row_at])
    return matrix

def derivative(field, axis_pick):
    matrix = jnp.asarray(diff_table(), dtype=jnp.float32)
    return jnp.einsum(EINSUM_FORMS[axis_pick], matrix, field, precision=lax.Precision.HIGHEST)

def face_slice(volume, face_index):
    endpoint = 4 * (face_index % 2)
    if face_index < 2:
        return volume[..., endpoint, :, :]
    if face_index < 4:
        return volume[..., :, endpoint, :]
    return volume[..., :, :, endpoint]

def put_face(volume, face_index, values):
    endpoint = 4 * (face_index % 2)
    if face_index < 2:
        return volume.at[..., endpoint, :, :].add(values)
    if face_index < 4:
        return volume.at[..., :, endpoint, :].add(values)
    return volume.at[..., :, :, endpoint].add(values)

def primitive(components):
    density = components[0]
    velocity = [components[1] / density, components[2] / density, components[3] / density]
    kinetic = 0.5 * (components[1] * velocity[0] + components[2] * velocity[1] + components[3] * velocity[2])
    pressure = (GAMMA - 1.0) * (components[4] - kinetic)
    return (velocity, pressure, pressure / density)

def inviscid(components, axis_pick):
    velocity, pressure, temper = primitive(components)
    normal_speed = velocity[axis_pick]
    result = [components[1 + axis_pick]]
    for member in range(3):
        flux_term = components[1 + member] * normal_speed
        if member == axis_pick:
            flux_term = flux_term + pressure
        result.append(flux_term)
    result.append((components[4] + pressure) * normal_speed)
    return result

def viscous(components, gradients, axis_pick):
    velocity, pressure, temper = primitive(components)
    divergence = gradients[0][0] + gradients[1][1] + gradients[2][2]
    stresses = []
    for member in range(3):
        stress = gradients[axis_pick][member] + gradients[member][axis_pick]
        if member == axis_pick:
            stress = stress - 2.0 / 3.0 * divergence
        stresses.append(VISC * stress)
    energy = stresses[0] * velocity[0] + stresses[1] * velocity[1] + stresses[2] * velocity[2] + COND * gradients[axis_pick][3]
    return [jnp.zeros_like(energy)] + stresses + [energy]

def wave_square(components):
    velocity, pressure, temper = primitive(components)
    return velocity[0] * velocity[0] + velocity[1] * velocity[1] + velocity[2] * velocity[2] + GAMMA * temper

def lifted_gradient(volume, outside, scales):
    components = [volume[..., member, :, :, :] for member in range(5)]
    velocity, pressure, temper = primitive(components)
    fields = velocity + [temper]
    outer_fields = []
    for face_index in range(6):
        outer_parts = [outside[face_index][..., member, :, :] for member in range(5)]
        outer_velocity, outer_pressure, outer_temper = primitive(outer_parts)
        outer_fields.append(outer_velocity + [outer_temper])
    gradients = []
    for axis_pick in range(3):
        factor = scales[..., axis_pick][..., None, None, None]
        grad_row = []
        for field_index in range(4):
            accumulated = derivative(fields[field_index], axis_pick)
            for upper_side in range(2):
                face_index = 2 * axis_pick + upper_side
                normal_sign = 2.0 * upper_side - 1.0
                trace_jump = outer_fields[face_index][field_index] - face_slice(fields[field_index], face_index)
                accumulated = put_face(accumulated, face_index, 0.5 * LIFT * normal_sign * trace_jump)
            grad_row.append(factor * accumulated)
        gradients.append(grad_row)
    return gradients

def own_viscous_faces(volume, gradients):
    components = [volume[..., member, :, :, :] for member in range(5)]
    result = []
    for face_index in range(6):
        face_parts = [face_slice(piece, face_index) for piece in components]
        face_grads = [[face_slice(entry, face_index) for entry in grad_row] for grad_row in gradients]
        result.append(jnp.stack(viscous(face_parts, face_grads, face_index // 2), axis=-3))
    return result

def residual_terms(volume, outside, gradients, visc_outside, scales, walls):
    components = [volume[..., member, :, :, :] for member in range(5)]
    totals = [jnp.zeros_like(components[0]) for member in range(5)]
    for axis_pick in range(3):
        factor = scales[..., axis_pick][..., None, None, None]
        convect = inviscid(components, axis_pick)
        diffuse = viscous(components, gradients, axis_pick)
        accumulated = [derivative(convect[member] - diffuse[member], axis_pick) for member in range(5)]
        for upper_side in range(2):
            face_index = 2 * axis_pick + upper_side
            normal_sign = 2.0 * upper_side - 1.0
            inner_parts = [face_slice(piece, face_index) for piece in components]
            outer_parts = [outside[face_index][..., member, :, :] for member in range(5)]
            outer_flux = inviscid(outer_parts, axis_pick)
            speed = jnp.sqrt(0.5 * (wave_square(inner_parts) + wave_square(outer_parts)))
            for member in range(5):
                inner_visc = face_slice(diffuse[member], face_index)
                outer_visc = visc_outside[face_index][..., member, :, :]
                if walls[face_index] is not None:
                    outer_visc = jnp.where(walls[face_index], inner_visc, outer_visc)
                surface = normal_sign * 0.5 * (outer_flux[member] - face_slice(convect[member], face_index)) - 0.5 * speed * (outer_parts[member] - inner_parts[member]) - normal_sign * 0.5 * (outer_visc - inner_visc)
                accumulated[member] = put_face(accumulated[member], face_index, LIFT * surface)
        totals = [totals[member] + factor * accumulated[member] for member in range(5)]
    return jnp.stack(totals, axis=-4)

def wall_masks(face_source):
    masks = [None, None, None, None, None, None]
    for face_index in (2, 3):
        masks[face_index] = (face_source[:, face_index] < 0)[:, None, None, None]
    return masks

def mirrored(face_trace):
    flips = 2.0 * (jnp.arange(5) % 4 == 0).astype(jnp.float32) - 1.0
    return face_trace * flips[:, None, None]

def pack_faces(volume):
    lead_shape = volume.shape[:2] + (-1,)
    return jnp.stack([face_slice(volume, face_index).reshape(lead_shape) for face_index in range(6)], axis=1)

def stack_faces(face_list):
    lead_shape = face_list[0].shape[:2] + (-1,)
    return jnp.stack([entry.reshape(lead_shape) for entry in face_list], axis=1)

def send_buffers(table, send_rows):
    picked = jnp.take(table, send_rows.reshape(-1), axis=0)
    return picked.reshape((2, send_rows.shape[2]) + table.shape[1:])

def pick_outside(table, received, face_source):
    whole = jnp.concatenate([table, received[0], received[3]], axis=0)
    picked = jnp.take(whole, jnp.maximum(face_source, 0).reshape(-1), axis=0)
    return picked.reshape(face_source.shape + table.shape[1:])

def split_traces(outside, upper_half, trailing):
    half_width = outside[0].shape[-1] // 2
    offset = half_width * upper_half
    return [entry[..., offset:offset + half_width].reshape(entry.shape[:-1] + trailing) for entry in outside]

def with_walls(outside, own_volume, walls):
    result = []
    for face_index in range(6):
        face_trace = outside[face_index]
        if walls[face_index] is not None:
            face_trace = jnp.where(walls[face_index][..., None], mirrored(face_slice(own_volume, face_index)), face_trace)
        result.append(face_trace)
    return result

def plane_reference(own_faces, face_source, send_rows):
    devices = send_rows.shape[0]
    table = own_faces[:, :4].reshape((devices, -1) + own_faces.shape[2:])
    buffers = jax.vmap(send_buffers)(table, send_rows[:, None])
    received = jnp.stack([jnp.roll(buffers[:, 1], 1, axis=0), buffers[:, 0], buffers[:, 1], jnp.roll(buffers[:, 0], -1, axis=0)], axis=1)
    plane = jax.vmap(pick_outside)(table, received, face_source.reshape(devices, -1, 4))
    plane = plane.reshape((-1,) + plane.shape[2:])
    return [plane[:, 0], plane[:, 1], plane[:, 2], plane[:, 3]]

def reference(state, direction, metric, face_source, send_rows):
    element = (5, 5, 5, 5)
    primal = jnp.moveaxis(state.reshape((PLANE, LAYERS) + element), 1, 0)[:, :, None]
    tangent = jnp.moveaxis(direction.reshape((PLANE, LAYERS) + element), 1, 0)[:, :, None]
    scales = jnp.moveaxis(metric, 1, 0)[:, :, None]
    walls = wall_masks(face_source)
    lead_shape = (LAYERS, PLANE, 1, -1)
    bottoms = jnp.concatenate([face_slice(primal, 4).reshape(lead_shape), face_slice(tangent, 4).reshape(lead_shape)], axis=-1)
    tops = jnp.concatenate([face_slice(primal, 5).reshape(lead_shape), face_slice(tangent, 5).reshape(lead_shape)], axis=-1)
    below_states = jnp.roll(tops, 1, axis=0)
    above_states = jnp.roll(bottoms, -1, axis=0)

    def first_section(volume_p, volume_t, scales_layer, below, above):
        own_states = jnp.concatenate([pack_faces(volume_p), pack_faces(volume_t)], axis=-1)
        outside = plane_reference(own_states, face_source, send_rows) + [below, above]
        outside_p = with_walls(split_traces(outside, 0, (5, 5, 5)), volume_p, walls)
        outside_t = with_walls(split_traces(outside, 1, (5, 5, 5)), volume_t, walls)
        grad_p, grad_t = jax.jvp(lambda volume, outer_side: lifted_gradient(volume, outer_side, scales_layer), (volume_p, outside_p), (volume_t, outside_t))
        return (outside_p, outside_t, grad_p, grad_t)

    def visc_section(inputs):
        volume_p, volume_t, scales_layer, below, above = inputs
        outside_p, outside_t, grad_p, grad_t = first_section(volume_p, volume_t, scales_layer, below, above)
        visc_p, visc_t = jax.jvp(own_viscous_faces, (volume_p, grad_p), (volume_t, grad_t))
        return jnp.concatenate([stack_faces(visc_p), stack_faces(visc_t)], axis=-1)
    own_visc = lax.map(visc_section, (primal, tangent, scales, below_states, above_states))
    visc_below = jnp.roll(own_visc[:, :, 5], 1, axis=0)
    visc_above = jnp.roll(own_visc[:, :, 4], -1, axis=0)

    def final_section(inputs):
        volume_p, volume_t, scales_layer, below, above, visc_own, visc_low, visc_high = inputs
        outside_p, outside_t, grad_p, grad_t = first_section(volume_p, volume_t, scales_layer, below, above)
        visc_out = plane_reference(visc_own, face_source, send_rows) + [visc_low, visc_high]
        visc_p = split_traces(visc_out, 0, (5, 5, 5))
        visc_t = split_traces(visc_out, 1, (5, 5, 5))
        return jax.jvp(lambda volume, outer_side, gradients, visc_side: residual_terms(volume, outer_side, gradients, visc_side, scales_layer, walls), (volume_p, outside_p, grad_p, visc_p), (volume_t, outside_t, grad_t, visc_t))
    res_p, res_t = lax.map(final_section, (primal, tangent, scales, below_states, above_states, own_visc, visc_below, visc_above))
    residual = jnp.moveaxis(res_p[:, :, 0], 0, 1).reshape(state.shape)
    product = jnp.moveaxis(res_t[:, :, 0], 0, 1).reshape(state.shape)
    total = float(state.size)
    coefficient = jnp.sum(direction * product) / total
    remainder = product - coefficient * direction
    beta = jnp.sqrt(jnp.sum(remainder * remainder) / total)
    norm_value = jnp.sqrt(jnp.sum(residual * residual) / total)
    return (residual, remainder / beta, jnp.stack([coefficient, beta, norm_value]))
```

```python
import math

import jax
import jax.numpy as jnp
import numpy as np
from jax import lax
from jax.experimental import pallas as pl
from jax.experimental.pallas import tpu as pltpu
from jax.sharding import PartitionSpec as P

GAMMA = 1.4
VISC = 0.01
COND = VISC * GAMMA / ((GAMMA - 1.0) * 0.72)
HALF_LIFT = 5.0
F32 = jnp.float32
BF16 = jnp.bfloat16

C = 40
L = 2
R = C * L
SLOTS = 33
KCAT = 256
ROW_A = 4 * C
ROW_B = 5 * C


def diff_table():
    spread = math.sqrt(3.0 / 7.0)
    points = np.array([-1.0, -spread, 0.0, spread, 1.0])
    weights = np.array([np.prod([points[i] - points[j] for j in range(5) if j != i]) for i in range(5)])
    matrix = np.zeros((5, 5))
    for i in range(5):
        for j in range(5):
            if i != j:
                matrix[i, j] = weights[i] / (weights[j] * (points[i] - points[j]))
        matrix[i, i] = np.sum([1.0 / (points[i] - points[j]) for j in range(5) if j != i])
    return matrix


def face_nodes(face):
    axis, end = face // 2, 4 * (face % 2)
    grid = np.arange(125).reshape(5, 5, 5)
    return np.take(grid, end, axis=axis).reshape(-1)


def face_lane(face):
    return face * 25 if face < 4 else 128 + (face - 4) * 25


def tables():
    d = diff_table().astype(np.float32).astype(np.float64)
    eye = np.eye(5)
    sel = np.zeros((128, 256))
    for lane in list(range(100, 128)) + list(range(178, 256)):
        sel[0, lane] = 1.0
    sel_dir = np.zeros((3, 128, 256))
    lift = np.zeros((256, 3, 128))
    d_lift = np.zeros((3, 128, 128))
    kron = [np.kron(np.kron(d, eye), eye), np.kron(np.kron(eye, d), eye), np.kron(np.kron(eye, eye), d)]
    for a in range(3):
        d_lift[a, :125, :125] = kron[a].T
        for side in range(2):
            face = 2 * a + side
            sign = 2.0 * side - 1.0
            for n, node in enumerate(face_nodes(face)):
                lane = face_lane(face) + n
                sel[node, lane] = 1.0
                sel_dir[a, node, lane] = 1.0
                lift[lane, a, node] = HALF_LIFT * sign
                d_lift[a, node, node] -= HALF_LIFT * sign
    grad_xy = np.zeros((256, 256))
    grad_z = np.zeros((256, 128))
    for a in range(2):
        grad_xy[:128, a * 128 : (a + 1) * 128] = d_lift[a]
        grad_xy[128:, a * 128 : (a + 1) * 128] = lift[:128, a]
    grad_z[:128] = d_lift[2]
    grad_z[128:] = lift[128:, 2]
    scatter = (lift != 0).sum(axis=1).astype(np.float64)

    def halves(x):
        high = x.astype(jnp.bfloat16)
        low = (x - high.astype(np.float64)).astype(jnp.bfloat16)
        return high, low

    signs = np.zeros((8, 256))
    for face in range(6):
        lanes = slice(face_lane(face), face_lane(face) + 25)
        signs[0, lanes] = HALF_LIFT * (2.0 * (face % 2) - 1.0)
        signs[1, lanes] = HALF_LIFT
    return dict(
        sel=sel.astype(jnp.bfloat16),
        sel_dir=sel_dir.reshape(384, 256).astype(jnp.bfloat16),
        scatter=scatter.astype(jnp.bfloat16),
        grad_xy=halves(grad_xy),
        grad_z=halves(grad_z),
        div=halves(d_lift.reshape(384, 128)),
        signs=signs.astype(np.float32),
    )


CONST = tables()


def mm(a, b):
    return jnp.dot(a, b, preferred_element_type=F32)


def split2(x):
    high = x.astype(BF16)
    return high, (x - high.astype(F32)).astype(BF16)


def pick(x, ones, terms=3):
    total = None
    for _ in range(terms):
        part = x.astype(BF16)
        x = x - part.astype(F32)
        total = mm(part, ones) if total is None else total + mm(part, ones)
    return total


def choose(ones, x, terms=3):
    total = None
    for _ in range(terms):
        part = x.astype(BF16)
        x = x - part.astype(F32)
        total = mm(ones, part) if total is None else total + mm(ones, part)
    return total


def mm3(x, high, low):
    xh, xl = split2(x)
    return mm(xh, high) + mm(xl, high) + mm(xh, low)


def roll(x, shift):
    shift = shift % 128
    return pltpu.roll(x, shift, 1) if shift else x


class Du:
    def __init__(self, p, t):
        self.p, self.t = p, t

    def __add__(self, o):
        return Du(self.p + o.p, self.t + o.t)

    def __sub__(self, o):
        return Du(self.p - o.p, self.t - o.t)

    def __mul__(self, o):
        if isinstance(o, Du):
            return Du(self.p * o.p, self.p * o.t + self.t * o.p)
        return Du(self.p * o, self.t * o)


def primitive(u):
    inv = 1.0 / u[0].p

    def over_density(x):
        value = x.p * inv
        return Du(value, (x.t - value * u[0].t) * inv)

    vel = [over_density(u[i]) for i in (1, 2, 3)]
    kinetic = (u[1] * vel[0] + u[2] * vel[1] + u[3] * vel[2]) * 0.5
    pressure = (u[4] - kinetic) * (GAMMA - 1.0)
    return vel, pressure, over_density(pressure)


def wave_square(vel, temper):
    return vel[0] * vel[0] + vel[1] * vel[1] + vel[2] * vel[2] + temper * GAMMA


def viscous(vel, q, a):
    div = q[0][0] + q[1][1] + q[2][2]
    stress = []
    for b in range(3):
        s = q[a][b] + q[b][a]
        if b == a:
            s = s - div * (2.0 / 3.0)
        stress.append(s * VISC)
    energy = stress[0] * vel[0] + stress[1] * vel[1] + stress[2] * vel[2] + q[a][3] * COND
    return stress + [energy]


def block(start):
    return pl.ds(pl.multiple_of(start, 8), 8)


def lanes(width=128):
    return lax.broadcasted_iota(jnp.int32, (8, width), 1)


def own_keys(width):
    j = lax.broadcasted_iota(jnp.int32, (1, width), 1)
    g = (j >= C).astype(jnp.int32) + (j >= 2 * C).astype(jnp.int32) + (j >= 3 * C).astype(jnp.int32)
    return j, 4 * (j - C * g) + g


def parity(axis):
    return lax.rem(lax.axis_index(axis), 2) == 0


def fill_table(face_ref, tab_ref, count):
    lane = lanes()

    def body(cb, carry):
        for pt in range(2):
            for l in range(L):
                tiles = [face_ref[block((pt * count + v) * R + l * C + cb * 8), :128] for v in range(count)]
                for g in range(4):
                    acc = roll(tiles[0], -25 * g)
                    for v in range(1, count):
                        acc = jnp.where(lane >= 25 * v, roll(tiles[v], 25 * (v - g)), acc)
                    tab_ref[block(g * C + cb * 8), (pt * L + l) * 128 : (pt * L + l + 1) * 128] = acc
        return carry

    lax.fori_loop(0, C // 8, body, 0)


def send_parts(send_ref, face_ref, tab_ref, be_ref, bo_ref, ze_ref, zo_ref, count):
    even = parity("stream")
    low = send_ref[0, 0:1, :].astype(F32)
    up = send_ref[0, 1:2, :].astype(F32)
    first = jnp.where(even, up, low)
    second = jnp.where(even, low, up)
    diagonal = lax.broadcasted_iota(jnp.int32, (C, SLOTS), 0) == lax.broadcasted_iota(jnp.int32, (C, SLOTS), 1)
    _, keys = own_keys(4 * C)
    keys = keys.astype(F32)
    ones = []
    for row in (first, second):
        col = jnp.sum(jnp.where(diagonal, row, 0.0), axis=1, keepdims=True)
        ones.append((col == keys).astype(BF16))
    sent = choose(jnp.concatenate(ones, axis=0), tab_ref[...])
    be_ref[...] = sent[:SLOTS]
    bo_ref[...] = sent[C : C + SLOTS]
    even_z = parity("span")
    lane = lanes()

    def body(cb, carry):
        for pt in range(2):
            edge = []
            for z, l in ((0, 0), (1, L - 1)):
                tiles = [face_ref[block((pt * count + v) * R + l * C + cb * 8), 128:] for v in range(count)]
                acc = roll(tiles[0], -25 * z)
                for v in range(1, count):
                    acc = jnp.where(lane >= 25 * v, roll(tiles[v], 25 * (v - z)), acc)
                edge.append(acc)
            cols = slice(pt * 128, (pt + 1) * 128)
            ze_ref[block(cb * 8), cols] = jnp.where(even_z, edge[1], edge[0])
            zo_ref[block(cb * 8), cols] = jnp.where(even_z, edge[0], edge[1])
        return carry

    lax.fori_loop(0, C // 8, body, 0)


def fetch_outside(fs_ref, tab_ref, re_ref, ro_ref, rze_ref, rzo_ref, face_ref, cat, got, out, count, flips):
    even = parity("stream")
    j, keys = own_keys(KCAT)
    first = j - ROW_A + 4 * C
    second = j - ROW_B + 4 * C
    first = jnp.where(even, first + SLOTS, first)
    second = jnp.where(even, second, second + SLOTS)
    keys = jnp.where(j < ROW_A, keys, jnp.where(j < ROW_A + SLOTS, first, jnp.where((j >= ROW_B) & (j < ROW_B + SLOTS), second, -5)))
    ones = jnp.concatenate([(fs_ref[:, f : f + 1] == keys).astype(BF16) for f in range(4)], axis=0)
    cat[:ROW_A, :] = tab_ref[...]
    cat[ROW_A:, :] = jnp.zeros((KCAT - ROW_A, 512), F32)
    cat[ROW_A : ROW_A + SLOTS, :] = re_ref[...]
    cat[ROW_B : ROW_B + SLOTS, :] = ro_ref[...]
    got[...] = choose(ones, cat[...])
    even_z = parity("span")
    lane = lanes()

    def body(cb, carry):
        walls = [fs_ref[block(cb * 8), f : f + 1] < 0 for f in (2, 3)]
        own = (lane >= 100) | (walls[0] & (lane >= 50) & (lane < 75)) | (walls[1] & (lane >= 75))
        for pt in range(2):
            cols = slice(pt * 128, (pt + 1) * 128)
            from_e, from_o = rze_ref[block(cb * 8), cols], rzo_ref[block(cb * 8), cols]
            above = jnp.where(even_z, from_e, from_o)
            below = jnp.where(even_z, from_o, from_e)
            for l in range(L):
                tile = slice((pt * L + l) * 128, (pt * L + l + 1) * 128)
                picked = [got[block(f * C + cb * 8), tile] for f in range(4)]
                for v in range(count):
                    rows = block((pt * count + v) * R + l * C + cb * 8)
                    acc = roll(picked[0], -25 * v)
                    for f in range(1, 4):
                        acc = jnp.where(lane >= 25 * f, roll(picked[f], 25 * (f - v)), acc)
                    mine = face_ref[rows, :128]
                    out[rows, :128] = jnp.where(own, -mine if flips and v in (1, 2, 3) else mine, acc)
                    here = face_ref[rows, 128:]
                    other = face_ref[block((pt * count + v) * R + (1 - l) * C + cb * 8), 128:]
                    if l == 0:
                        lower, upper = roll(below, -25 * v), roll(other, 25)
                    else:
                        lower, upper = roll(other, -25), roll(above, 25 - 25 * v)
                    out[rows, 128:] = jnp.where(lane < 25, lower, jnp.where(lane < 50, upper, here))
        return carry

    lax.fori_loop(0, C // 8, body, 0)


def traces_kernel(state_ref, dir_ref, metric_ref, send_ref, sel_ref, u_ref, fl_ref, tab_ref, m_ref, be_ref, bo_ref, ze_ref, zo_ref, xs):
    lane = lanes()
    xs[:, 512:640] = jnp.zeros((2 * R, 128), F32)
    for pt, ref in enumerate((state_ref, dir_ref)):
        for l in range(L):
            xs[pt * R + l * C : pt * R + (l + 1) * C, 0:625] = ref[:, l, :]
    for l in range(L):
        m_ref[l * C : (l + 1) * C, 0:3] = metric_ref[:, l, :]
    for pt in range(2):

        def body(rb, carry):
            tiles = [xs[block(pt * R + rb * 8), t * 128 : (t + 1) * 128] for t in range(5)]
            for v in range(5):
                value = roll(tiles[v], 3 * v)
                if v:
                    value = jnp.where(lane < 3 * v, roll(tiles[v - 1], 3 * v), value)
                pad = 1.0 if pt == 0 and v in (0, 4) else 0.0
                u_ref[block((pt * 5 + v) * R + rb * 8), :] = jnp.where(lane < 125, value, pad)
            return carry

        lax.fori_loop(0, R // 8, body, 0)
    fl_ref[...] = pick(u_ref[...], sel_ref[...])
    fill_table(fl_ref, tab_ref, 5)
    send_parts(send_ref, fl_ref, tab_ref, be_ref, bo_ref, ze_ref, zo_ref, 5)


def load(ref, count, rows, cols):
    return [Du(ref[block(v * R + rows), cols], ref[block((count + v) * R + rows), cols]) for v in range(count)]


def store(ref, count, v, rows, cols, value):
    ref[block(v * R + rows), cols] = value.p
    ref[block((count + v) * R + rows), cols] = value.t


ALL = slice(None)


def gradient_kernel(
    fs_ref, send_ref, u_ref, fl_ref, tab_ref, m_ref, re_ref, ro_ref, rze_ref, rzo_ref,
    gxh_ref, gxl_ref, gzh_ref, gzl_ref, sd_ref,
    out_ref, q_ref, vfl_ref, vtab_ref, be_ref, bo_ref, ze_ref, zo_ref,
    cat, got, w, wo, vv,
):
    fetch_outside(fs_ref, tab_ref, re_ref, ro_ref, rze_ref, rzo_ref, fl_ref, cat, got, out_ref, 5, True)

    def fields(rb, carry):
        rows = rb * 8
        for src, dst in ((u_ref, w), (out_ref, wo)):
            vel, _, temper = primitive(load(src, 5, rows, ALL))
            for f, value in enumerate(vel + [temper]):
                store(dst, 4, f, rows, ALL, value)
        return carry

    lax.fori_loop(0, R // 8, fields, 0)
    wh, wl = split2(w[...])
    oh, ol = split2(wo[...])
    xyh = jnp.concatenate([wh, oh[:, :128]], axis=1)
    xyl = jnp.concatenate([wl, ol[:, :128]], axis=1)
    zh = jnp.concatenate([wh, oh[:, 128:]], axis=1)
    zl = jnp.concatenate([wl, ol[:, 128:]], axis=1)
    q_ref[:, :256] = mm(xyh, gxh_ref[...]) + mm(xyl, gxh_ref[...]) + mm(xyh, gxl_ref[...])
    q_ref[:, 256:] = mm(zh, gzh_ref[...]) + mm(zl, gzh_ref[...]) + mm(zh, gzl_ref[...])

    def stresses(rb, carry):
        rows = rb * 8
        vel = [Du(w[block(f * R + rows), :], w[block((4 + f) * R + rows), :]) for f in range(3)]
        q = []
        for a in range(3):
            scale = m_ref[block(rows), a : a + 1]
            q.append([d * scale for d in load(q_ref, 4, rows, slice(a * 128, (a + 1) * 128))])
        for a in range(3):
            for v, value in enumerate(viscous(vel, q, a)):
                store(vv, 4, v, rows, slice(a * 128, (a + 1) * 128), value)
        return carry

    lax.fori_loop(0, R // 8, stresses, 0)
    q_ref[...] = vv[...]
    vfl_ref[...] = pick(vv[...], sd_ref[...], 2)
    fill_table(vfl_ref, vtab_ref, 4)
    send_parts(send_ref, vfl_ref, vtab_ref, be_ref, bo_ref, ze_ref, zo_ref, 4)


def inner_kernel(u_ref, fl_ref, out_ref, vv_ref, m_ref, sg_ref, dh_ref, dl_ref, part_ref, surf_ref, ms_ref, fv):
    lane = lanes(256)

    def volume(rb, carry):
        rows = rb * 8
        u = load(u_ref, 5, rows, ALL)
        vel, pressure, _ = primitive(u)
        total = u[4] + pressure
        for a in range(3):
            cols = slice(a * 128, (a + 1) * 128)
            scale = m_ref[block(rows), a : a + 1]
            visc = load(vv_ref, 4, rows, cols)
            store(fv, 5, 0, rows, cols, u[1 + a] * scale)
            for i in range(3):
                flux = u[1 + i] * vel[a]
                if i == a:
                    flux = flux + pressure
                store(fv, 5, 1 + i, rows, cols, (flux - visc[i]) * scale)
            store(fv, 5, 4, rows, cols, (total * vel[a] - visc[3]) * scale)
        return carry

    lax.fori_loop(0, R // 8, volume, 0)
    part_ref[...] = mm3(fv[...], dh_ref[...], dl_ref[...])

    def by_lane(x, y, z):
        return jnp.where(lane < 50, x, jnp.where(lane < 128, y, z))

    def normal(vals):
        return Du(by_lane(*[d.p for d in vals]), by_lane(*[d.t for d in vals]))

    def surface(rb, carry):
        rows = rb * 8
        inner = load(fl_ref, 5, rows, ALL)
        vel, _, temper = primitive(inner)
        speed2 = wave_square(vel, temper)
        outer = load(out_ref, 5, rows, ALL)
        vel, pressure, temper = primitive(outer)
        speed2 = (speed2 + wave_square(vel, temper)) * 0.5
        root = jnp.sqrt(speed2.p)
        speed = Du(root, 0.5 * speed2.t / root)
        mface = by_lane(*[m_ref[block(rows), a : a + 1] for a in range(3)])
        lift_s = sg_ref[0:1, :] * mface
        lift = sg_ref[1:2, :] * mface
        ms_ref[block(rows), :] = lift_s
        speed = speed * lift
        vn = normal(vel)
        fluxes = [normal(outer[1:4])]
        for i in range(3):
            flux = outer[1 + i] * vn
            side = (lane < 50) if i == 0 else ((lane >= 50) & (lane < 128)) if i == 1 else (lane >= 128)
            fluxes.append(Du(flux.p + jnp.where(side, pressure.p, 0.0), flux.t + jnp.where(side, pressure.t, 0.0)))
        fluxes.append((outer[4] + pressure) * vn)
        for v in range(5):
            store(surf_ref, 5, v, rows, ALL, fluxes[v] * lift_s - speed * (outer[v] - inner[v]))
        return carry

    lax.fori_loop(0, R // 8, surface, 0)


def unpack(tiles, lane, t):
    value = roll(tiles[t], -3 * t)
    if t < 4:
        value = jnp.where(lane < 125 - 3 * t, value, roll(tiles[t + 1], -3 * (t + 1)))
    return value


def final_kernel(
    fs_ref, vtab_ref, re_ref, ro_ref, rze_ref, rzo_ref, vfl_ref, part_ref, surf_ref, ms_ref, u_ref, sc_ref,
    res_ref, prod_ref, sums_ref,
    cat, got, vo, sf, xs,
):
    fetch_outside(fs_ref, vtab_ref, re_ref, ro_ref, rze_ref, rzo_ref, vfl_ref, cat, got, vo, 4, False)

    def surface(rb, carry):
        rows = rb * 8
        scale = ms_ref[block(rows), :]
        for pt in range(2):
            sf[block(pt * 5 * R + rows), :] = surf_ref[block(pt * 5 * R + rows), :]
            for v in range(4):
                at = block((pt * 5 + 1 + v) * R + rows)
                sf[at, :] = surf_ref[at, :] - scale * vo[block((pt * 4 + v) * R + rows), :]
        return carry

    lax.fori_loop(0, R // 8, surface, 0)
    sf[:, :128] = part_ref[...] + pick(sf[...], sc_ref[...], 2)
    lane = lanes()

    def output(rb, sums):
        sums = list(sums)
        rows = rb * 8
        prod = []
        for pt in range(2):
            tiles = [sf[block((pt * 5 + v) * R + rows), :128] for v in range(5)]
            tiles = [jnp.where(lane < 125, x, 0.0) for x in tiles]
            for t in range(5):
                xs[block(pt * R + rows), t * 128 : (t + 1) * 128] = unpack(tiles, lane, t)
            prod.append(tiles)
        for v in range(5):
            d = u_ref[block((5 + v) * R + rows), :]
            res, p = prod[0][v], prod[1][v]
            for i, x in enumerate((d * p, d * d, res * res, p * p)):
                sums[i] = sums[i] + x
        return tuple(sums)

    zero = jnp.zeros((8, 128), F32)
    sums = lax.fori_loop(0, R // 8, output, (zero, zero, zero, zero))
    lane1 = lax.broadcasted_iota(jnp.int32, (1, 128), 1)
    row = jnp.zeros((1, 128), F32)
    for i, x in enumerate(sums):
        x = jnp.sum(jnp.sum(x, axis=0, keepdims=True), axis=1, keepdims=True)
        row = jnp.where(lane1 == i, x, row)
    sums_ref[...] = row
    for pt, ref in enumerate((res_ref, prod_ref)):
        for l in range(L):
            ref[:, l, :] = xs[pt * R + l * C : pt * R + (l + 1) * C, 0:625]


def scale_kernel(all_ref, prod_ref, dir_ref, basis_ref, krylov_ref, *, total):
    sums = jnp.sum(all_ref[...], axis=0, keepdims=True)
    dp, dd, rr, pp = [sums[:, i : i + 1] for i in range(4)]
    coefficient = dp / total
    beta = jnp.sqrt((pp - 2.0 * coefficient * dp + coefficient * coefficient * dd) / total)
    norm = jnp.sqrt(rr / total)
    lane1 = lax.broadcasted_iota(jnp.int32, (1, 128), 1)
    krylov_ref[...] = jnp.where(lane1 == 0, coefficient, jnp.where(lane1 == 1, beta, norm))
    basis_ref[...] = (prod_ref[...] - coefficient.reshape(1, 1, 1) * dir_ref[...]) / beta.reshape(1, 1, 1)


def shaped(*dims):
    return jax.ShapeDtypeStruct(dims, F32)


def vmem(*dims):
    return pltpu.VMEM(dims, F32)


def pairs_of(count):
    first = [(i, i ^ 1) for i in range(count)]
    second = [(i, (((i + 1) ^ 1) - 1) % count) for i in range(count)]
    return first, second


def exchange(be, bo, ze, zo):
    se, so = pairs_of(lax.axis_size("stream"))
    pe, po = pairs_of(lax.axis_size("span"))
    return (
        lax.ppermute(be, "stream", se),
        lax.ppermute(bo, "stream", so),
        lax.ppermute(ze, "span", pe),
        lax.ppermute(zo, "span", po),
    )


SENT = (shaped(SLOTS, 512), shaped(SLOTS, 512), shaped(C, 256), shaped(C, 256))


def local(state, direction, metric, face_source, send_rows):
    u, fl, tab, m, *sent = pl.pallas_call(
        traces_kernel,
        out_shape=(shaped(10 * R, 128), shaped(10 * R, 256), shaped(4 * C, 512), shaped(R, 128)) + SENT,
        scratch_shapes=[vmem(2 * R, 640)],
        name="traces",
    )(state, direction, metric, send_rows, CONST["sel"])
    got = exchange(*sent)
    out, vv, vfl, vtab, *sent = pl.pallas_call(
        gradient_kernel,
        out_shape=(shaped(10 * R, 256), shaped(8 * R, 384), shaped(8 * R, 256), shaped(4 * C, 512)) + SENT,
        scratch_shapes=[vmem(KCAT, 512), vmem(4 * C, 512), vmem(8 * R, 128), vmem(8 * R, 256), vmem(8 * R, 384)],
        name="gradient",
    )(face_source, send_rows, u, fl, tab, m, *got, *CONST["grad_xy"], *CONST["grad_z"], CONST["sel_dir"])
    got = exchange(*sent)
    part, surf, ms = pl.pallas_call(
        inner_kernel,
        out_shape=(shaped(10 * R, 128), shaped(10 * R, 256), shaped(R, 256)),
        scratch_shapes=[vmem(10 * R, 384)],
        name="inner",
    )(u, fl, out, vv, m, CONST["signs"], *CONST["div"])
    residual, product, sums = pl.pallas_call(
        final_kernel,
        out_shape=(shaped(C, L, 625), shaped(C, L, 625), shaped(1, 128)),
        scratch_shapes=[vmem(KCAT, 512), vmem(4 * C, 512), vmem(8 * R, 256), vmem(10 * R, 256), vmem(2 * R, 640)],
        name="final",
    )(face_source, vtab, *got, vfl, part, surf, ms, u, CONST["scatter"])
    axes = ("stream", "span")
    count = lax.axis_size("stream") * lax.axis_size("span")
    spread = jnp.broadcast_to(sums[None], (count, 1, 128))
    everyone = lax.all_to_all(spread, axes, 0, 0, tiled=True).reshape(count, 128)
    total = float(state.size * count)
    basis, krylov = pl.pallas_call(
        lambda *refs: scale_kernel(*refs, total=total),
        out_shape=(shaped(C, L, 625), shaped(1, 128)),
        name="scale",
    )(everyone, product, direction)
    return residual, basis, krylov[0, :3]


def solution(mesh):
    cells = P("stream", "span", None)
    in_specs = (cells, cells, cells, P("stream", None), P("stream", None, None))
    out_specs = (cells, cells, P())
    return jax.shard_map(local, mesh=mesh, in_specs=in_specs, out_specs=out_specs, check_vma=False)
```

```python
import math

import jax
import jax.numpy as jnp
import numpy as np
from jax import lax
from jax.experimental import pallas as pl
from jax.experimental.pallas import tpu as pltpu
from jax.sharding import PartitionSpec as P

GAMMA = 1.4
VISC = 0.01
COND = VISC * GAMMA / ((GAMMA - 1.0) * 0.72)
HALF_LIFT = 5.0
F32 = jnp.float32
BF16 = jnp.bfloat16

C = 40
L = 2
R = C * L
SLOTS = 33


def diff_table():
    spread = math.sqrt(3.0 / 7.0)
    points = np.array([-1.0, -spread, 0.0, spread, 1.0])
    weights = np.array([np.prod([points[i] - points[j] for j in range(5) if j != i]) for i in range(5)])
    matrix = np.zeros((5, 5))
    for i in range(5):
        for j in range(5):
            if i != j:
                matrix[i, j] = weights[i] / (weights[j] * (points[i] - points[j]))
        matrix[i, i] = np.sum([1.0 / (points[i] - points[j]) for j in range(5) if j != i])
    return matrix


def face_nodes(face):
    axis, end = face // 2, 4 * (face % 2)
    grid = np.arange(125).reshape(5, 5, 5)
    return np.take(grid, end, axis=axis).reshape(-1)


def face_lane(face):
    return face * 25 if face < 4 else 128 + (face - 4) * 25


def tables():
    d = diff_table().astype(np.float32).astype(np.float64)
    eye = np.eye(5)
    sel = np.zeros((128, 256))
    for lane in list(range(100, 128)) + list(range(178, 256)):
        sel[0, lane] = 1.0
    trace = np.zeros((640, 768))
    trace_v = np.zeros((3, 512, 256))
    place_v = np.zeros((768, 512))
    lift = np.zeros((256, 3, 128))
    d_lift = np.zeros((3, 128, 128))
    kron = [np.kron(np.kron(d, eye), eye), np.kron(np.kron(eye, d), eye), np.kron(np.kron(eye, eye), d)]
    signs = np.zeros((8, 256))
    for a in range(3):
        d_lift[a, :125, :125] = kron[a].T
        for side in range(2):
            face = 2 * a + side
            sign = 2.0 * side - 1.0
            signs[0, face_lane(face) : face_lane(face) + 25] = HALF_LIFT * sign
            signs[1, face_lane(face) : face_lane(face) + 25] = HALF_LIFT
            for n, node in enumerate(face_nodes(face)):
                lane = face_lane(face) + n
                sel[node, lane] = 1.0
                lift[lane, a, node] = HALF_LIFT * sign
                d_lift[a, node, node] -= HALF_LIFT * sign
                for v in range(5):
                    trace[v * 125 + node, face * 128 + v * 25 + n] = 1.0
                for v in range(4):
                    trace_v[a, v * 128 + node, side * 128 + v * 25 + n] = 1.0
                    place_v[face * 128 + v * 25 + n, v * 128 + node] = 1.0
    scatter = (lift != 0).sum(axis=1).astype(np.float64)

    def halves(x):
        high = x.astype(jnp.bfloat16)
        low = (x - high.astype(np.float64)).astype(jnp.bfloat16)
        return np.concatenate([high, low], axis=0)

    return dict(
        trace=trace.astype(jnp.bfloat16),
        sel=sel.astype(jnp.bfloat16),
        grad=halves(np.concatenate(list(d_lift), axis=1)),
        lift_xy=np.concatenate([lift[:128, 0], lift[:128, 1]], axis=1).astype(jnp.bfloat16),
        lift_z=lift[128:, 2].astype(jnp.bfloat16),
        trace_v=trace_v.reshape(1536, 256).astype(jnp.bfloat16),
        place_v=place_v.astype(jnp.bfloat16),
        scatter=scatter.astype(jnp.bfloat16),
        div=halves(d_lift.reshape(384, 128)),
        signs=signs.astype(np.float32),
    )


CONST = tables()


def mm(a, b):
    return jnp.dot(a, b, preferred_element_type=F32)


def split2(x):
    high = x.astype(BF16)
    return high, (x - high.astype(F32)).astype(BF16)


def pick(x, ones, terms=3):
    total = None
    for _ in range(terms):
        part = x.astype(BF16)
        x = x - part.astype(F32)
        total = mm(part, ones) if total is None else total + mm(part, ones)
    return total


def choose(ones, x, terms=3):
    total = None
    for _ in range(terms):
        part = x.astype(BF16)
        x = x - part.astype(F32)
        total = mm(ones, part) if total is None else total + mm(ones, part)
    return total


def mm3(x, high, low):
    xh, xl = split2(x)
    return mm(xh, high) + mm(xl, high) + mm(xh, low)


def roll(x, shift):
    shift = shift % 128
    return pltpu.roll(x, shift, 1) if shift else x


class Du:
    def __init__(self, p, t):
        self.p, self.t = p, t

    def __add__(self, o):
        return Du(self.p + o.p, self.t + o.t)

    def __sub__(self, o):
        return Du(self.p - o.p, self.t - o.t)

    def __mul__(self, o):
        if isinstance(o, Du):
            return Du(self.p * o.p, self.p * o.t + self.t * o.p)
        return Du(self.p * o, self.t * o)


def primitive(u):
    inv = 1.0 / u[0].p

    def over_density(x):
        value = x.p * inv
        return Du(value, (x.t - value * u[0].t) * inv)

    vel = [over_density(u[i]) for i in (1, 2, 3)]
    kinetic = (u[1] * vel[0] + u[2] * vel[1] + u[3] * vel[2]) * 0.5
    pressure = (u[4] - kinetic) * (GAMMA - 1.0)
    return vel, pressure, over_density(pressure)


def wave_square(vel, temper):
    return vel[0] * vel[0] + vel[1] * vel[1] + vel[2] * vel[2] + temper * GAMMA


def viscous(vel, q, a):
    div = q[0][0] + q[1][1] + q[2][2]
    stress = []
    for b in range(3):
        s = q[a][b] + q[b][a]
        if b == a:
            s = s - div * (2.0 / 3.0)
        stress.append(s * VISC)
    energy = stress[0] * vel[0] + stress[1] * vel[1] + stress[2] * vel[2] + q[a][3] * COND
    return stress + [energy]


def block(start):
    return pl.ds(pl.multiple_of(start, 8), 8)


def lanes(width=128):
    return lax.broadcasted_iota(jnp.int32, (8, width), 1)


def parity(axis):
    return lax.rem(lax.axis_index(axis), 2) == 0


def own_keys(width):
    j = lax.broadcasted_iota(jnp.int32, (1, width), 1)
    g = (j >= C).astype(jnp.int32) + (j >= 2 * C).astype(jnp.int32) + (j >= 3 * C).astype(jnp.int32)
    return (4 * (j - C * g) + g).astype(F32)


def column(row):
    shape = (C, row.shape[1])
    diagonal = lax.broadcasted_iota(jnp.int32, shape, 0) == lax.broadcasted_iota(jnp.int32, shape, 1)
    return jnp.sum(jnp.where(diagonal, row, 0.0), axis=1, keepdims=True)


def tile_of(pt, l):
    return slice((pt * L + l) * 128, (pt * L + l + 1) * 128)


def send_parts(send_ref, tab_ref, be_ref, bo_ref, ze_ref, zo_ref, terms):
    even = parity("stream")
    low = send_ref[0, 0:1, :].astype(F32)
    up = send_ref[0, 1:2, :].astype(F32)
    keys = own_keys(4 * C)
    ones = [
        (column(jnp.where(even, x, y)) == keys).astype(BF16) for x, y in ((up, low), (low, up))
    ]
    sent = choose(jnp.concatenate(ones, axis=0), tab_ref[: 4 * C, :], terms)
    be_ref[...] = sent[:SLOTS]
    bo_ref[...] = sent[C : C + SLOTS]
    even_z = parity("span")
    for pt in range(2):
        bottom = tab_ref[4 * C : 5 * C, tile_of(pt, 0)]
        top = tab_ref[5 * C : 6 * C, tile_of(pt, L - 1)]
        cols = slice(pt * 128, (pt + 1) * 128)
        ze_ref[:, cols] = jnp.where(even_z, top, bottom)
        zo_ref[:, cols] = jnp.where(even_z, bottom, top)


def join_received(rcv, re_ref, ro_ref):
    rcv[...] = jnp.zeros(rcv.shape, F32)
    rcv[:SLOTS, :] = re_ref[...]
    rcv[C : C + SLOTS, :] = ro_ref[...]


def spanwise(tab_ref, rze_ref, rzo_ref, even_z, rows, pt, l):
    cols = slice(pt * 128, (pt + 1) * 128)
    if l == 0:
        lower = jnp.where(even_z, rzo_ref[block(rows), cols], rze_ref[block(rows), cols])
        return lower, tab_ref[block(4 * C + rows), tile_of(pt, 1)]
    upper = jnp.where(even_z, rze_ref[block(rows), cols], rzo_ref[block(rows), cols])
    return tab_ref[block(5 * C + rows), tile_of(pt, 0)], upper


def traces_kernel(state_hbm, dir_hbm, trace_hbm, send_ref, xs, tab_ref, be_ref, bo_ref, ze_ref, zo_ref, sbuf, dbuf, tbuf, sems):
    copies = [
        pltpu.make_async_copy(src, dst, sems.at[i])
        for i, (src, dst) in enumerate(((state_hbm, sbuf), (dir_hbm, dbuf), (trace_hbm, tbuf)))
    ]
    for copy in copies:
        copy.start()
    xs[:, 512:640] = jnp.zeros((2 * R, 128), F32)
    for pt, ref in enumerate((sbuf, dbuf)):
        copies[pt].wait()
        for l in range(L):
            xs[pt * R + l * C : pt * R + (l + 1) * C, 0:625] = ref[:, l, :]
    copies[2].wait()
    for i in range(3):
        faces = pick(xs[...], tbuf[:, i * 256 : (i + 1) * 256])
        for side in range(2):
            for pt in range(2):
                for l in range(L):
                    at = pt * R + l * C
                    tab_ref[(2 * i + side) * C : (2 * i + side + 1) * C, tile_of(pt, l)] = faces[at : at + C, side * 128 : (side + 1) * 128]
    send_parts(send_ref, tab_ref, be_ref, bo_ref, ze_ref, zo_ref, 3)


def load(ref, count, rows, cols):
    return [Du(ref[block(v * R + rows), cols], ref[block((count + v) * R + rows), cols]) for v in range(count)]


def store(ref, count, v, rows, cols, value):
    ref[block(v * R + rows), cols] = value.p
    ref[block((count + v) * R + rows), cols] = value.t


ALL = slice(None)


def before_kernel(xs, tab_ref, metric_ref, fs_ref, sel_ref, grad_ref, u_ref, fl_ref, w_ref, q_ref, m_ref, ones_ref, wall_ref, own_ref):
    lane = lanes()
    for pt in range(2):

        def body(rb, carry):
            tiles = [xs[block(pt * R + rb * 8), t * 128 : (t + 1) * 128] for t in range(5)]
            for v in range(5):
                value = roll(tiles[v], 3 * v)
                if v:
                    value = jnp.where(lane < 3 * v, roll(tiles[v - 1], 3 * v), value)
                pad = 1.0 if pt == 0 and v in (0, 4) else 0.0
                u_ref[block((pt * 5 + v) * R + rb * 8), :] = jnp.where(lane < 125, value, pad)
            return carry

        lax.fori_loop(0, R // 8, body, 0)
    for l in range(L):
        for a in range(3):
            m_ref[l * C : (l + 1) * C, a : a + 1] = column(metric_ref[a, l : l + 1, :])
    even = parity("stream")
    keys = own_keys(4 * C)
    j = lax.broadcasted_iota(jnp.int32, (1, 2 * C), 1)
    near = jnp.where(j < C, j, j - C)
    named = 4 * C + near + jnp.where((j < C) == even, SLOTS, 0)
    far = jnp.where(near < SLOTS, named, -5).astype(F32)
    at = lax.broadcasted_iota(jnp.int32, (C, 1), 0).astype(F32) * 4.0
    for f in range(4):
        col = column(fs_ref[f : f + 1, :].astype(F32))
        wall = col < 0.0
        col = jnp.where(wall, at + float(f), col)
        ones_ref[f * C : (f + 1) * C, 0 : 4 * C] = (col == keys).astype(BF16)
        ones_ref[f * C : (f + 1) * C, 256 : 256 + 2 * C] = (col == far).astype(BF16)
        wall_ref[f * C : (f + 1) * C, :] = jnp.broadcast_to(jnp.where(wall, -1.0, 1.0), (C, 128))
    own_ref[...] = choose(ones_ref[:, : 4 * C], tab_ref[: 4 * C, :])

    def fields(rb, carry):
        rows = rb * 8
        vel, _, temper = primitive(load(u_ref, 5, rows, ALL))
        for f, value in enumerate(vel + [temper]):
            store(w_ref, 4, f, rows, ALL, value)
        return carry

    lax.fori_loop(0, R // 8, fields, 0)
    q_ref[...] = mm3(w_ref[...], grad_ref[:128, :], grad_ref[128:, :])
    fl_ref[...] = pick(u_ref[...], sel_ref[...])


def gradient_kernel(
    send_ref, tab_ref, w_ref, q_ref, m_ref, ones_ref, wall_ref, own_ref, re_ref, ro_ref, rze_ref, rzo_ref,
    lxy_ref, lz_ref, tv_ref,
    out_ref, vv, vtab_ref, be_ref, bo_ref, ze_ref, zo_ref,
    rcv, got, wo, ql,
):
    join_received(rcv, re_ref, ro_ref)
    got[...] = own_ref[...] + choose(ones_ref[:, 256 : 256 + 2 * C], rcv[...])
    even_z = parity("span")
    lane = lanes()
    moment = (lane >= 25) & (lane < 100)

    def outside(cb, carry):
        rows = cb * 8
        flip = [None, None] + [jnp.where(moment, wall_ref[block(f * C + rows), :], 1.0) for f in (2, 3)]
        for l in range(L):
            state = []
            for pt in range(2):
                picked = [got[block(f * C + rows), tile_of(pt, l)] for f in range(4)]
                picked = [x if s is None else x * s for x, s in zip(picked, flip)]
                lower, upper = spanwise(tab_ref, rze_ref, rzo_ref, even_z, rows, pt, l)
                both = []
                for v in range(5):
                    at = block((pt * 5 + v) * R + l * C + rows)
                    pad = 1.0 if pt == 0 and v in (0, 4) else 0.0
                    acc = roll(picked[0], -25 * v)
                    for f in range(1, 4):
                        acc = jnp.where(lane >= 25 * f, roll(picked[f], 25 * (f - v)), acc)
                    acc = jnp.where(lane >= 100, pad, acc)
                    edge = jnp.where(lane < 25, roll(lower, -25 * v), jnp.where(lane < 50, roll(upper, 25 - 25 * v), pad))
                    out_ref[at, :128] = acc
                    out_ref[at, 128:] = edge
                    both.append((acc, edge))
                state.append(both)
            for half in range(2):
                u = [Du(state[0][v][half], state[1][v][half]) for v in range(5)]
                vel, _, temper = primitive(u)
                for f, value in enumerate(vel + [temper]):
                    store(wo, 4, f, l * C + rows, slice(half * 128, (half + 1) * 128), value)
        return carry

    lax.fori_loop(0, C // 8, outside, 0)
    ql[:, :256] = pick(wo[:, :128], lxy_ref[...], 2)
    ql[:, 256:] = pick(wo[:, 128:], lz_ref[...], 2)

    def stresses(rb, carry):
        rows = rb * 8
        vel = [Du(w_ref[block(f * R + rows), :], w_ref[block((4 + f) * R + rows), :]) for f in range(3)]
        q = []
        for a in range(3):
            scale = m_ref[block(rows), a : a + 1]
            cols = slice(a * 128, (a + 1) * 128)
            q.append([(x + y) * scale for x, y in zip(load(q_ref, 4, rows, cols), load(ql, 4, rows, cols))])
        for a in range(3):
            for v, value in enumerate(viscous(vel, q, a)):
                cols = slice((a * 4 + v) * 128, (a * 4 + v + 1) * 128)
                vv[block(rows), cols] = value.p
                vv[block(R + rows), cols] = value.t
        return carry

    lax.fori_loop(0, R // 8, stresses, 0)
    for a in range(3):
        faces = pick(vv[:, a * 512 : (a + 1) * 512], tv_ref[a * 512 : (a + 1) * 512, :], 2)
        for side in range(2):
            for pt in range(2):
                for l in range(L):
                    at = pt * R + l * C
                    vtab_ref[(2 * a + side) * C : (2 * a + side + 1) * C, tile_of(pt, l)] = faces[at : at + C, side * 128 : (side + 1) * 128]
    send_parts(send_ref, vtab_ref, be_ref, bo_ref, ze_ref, zo_ref, 2)


def inner_kernel(u_ref, fl_ref, out_ref, vv_ref, vtab_ref, ones_ref, m_ref, sg_ref, div_ref, sc_ref, part_ref, own_ref, fv, surf_ref):
    lane = lanes(256)
    own_ref[...] = choose(ones_ref[:, : 4 * C], vtab_ref[: 4 * C, :], 2)

    def volume(rb, carry):
        rows = rb * 8
        u = load(u_ref, 5, rows, ALL)
        vel, pressure, _ = primitive(u)
        total = u[4] + pressure
        for a in range(3):
            cols = slice(a * 128, (a + 1) * 128)
            scale = m_ref[block(rows), a : a + 1]
            visc = []
            for v in range(4):
                at = slice((a * 4 + v) * 128, (a * 4 + v + 1) * 128)
                visc.append(Du(vv_ref[block(rows), at], vv_ref[block(R + rows), at]))
            store(fv, 5, 0, rows, cols, u[1 + a] * scale)
            for i in range(3):
                flux = u[1 + i] * vel[a]
                if i == a:
                    flux = flux + pressure
                store(fv, 5, 1 + i, rows, cols, (flux - visc[i]) * scale)
            store(fv, 5, 4, rows, cols, (total * vel[a] - visc[3]) * scale)
        return carry

    lax.fori_loop(0, R // 8, volume, 0)

    def by_lane(x, y, z):
        return jnp.where(lane < 50, x, jnp.where(lane < 128, y, z))

    def normal(vals):
        return Du(by_lane(*[d.p for d in vals]), by_lane(*[d.t for d in vals]))

    def surface(rb, carry):
        rows = rb * 8
        inner = load(fl_ref, 5, rows, ALL)
        vel, _, temper = primitive(inner)
        speed2 = wave_square(vel, temper)
        outer = load(out_ref, 5, rows, ALL)
        vel, pressure, temper = primitive(outer)
        speed2 = (speed2 + wave_square(vel, temper)) * 0.5
        root = jnp.sqrt(speed2.p)
        speed = Du(root, 0.5 * speed2.t / root)
        mface = by_lane(*[m_ref[block(rows), a : a + 1] for a in range(3)])
        lift_s = sg_ref[0:1, :] * mface
        speed = speed * (sg_ref[1:2, :] * mface)
        vn = normal(vel)
        fluxes = [normal(outer[1:4])]
        for i in range(3):
            flux = outer[1 + i] * vn
            side = (lane < 50) if i == 0 else ((lane >= 50) & (lane < 128)) if i == 1 else (lane >= 128)
            fluxes.append(Du(flux.p + jnp.where(side, pressure.p, 0.0), flux.t + jnp.where(side, pressure.t, 0.0)))
        fluxes.append((outer[4] + pressure) * vn)
        for v in range(5):
            store(surf_ref, 5, v, rows, ALL, fluxes[v] * lift_s - speed * (outer[v] - inner[v]))
        return carry

    lax.fori_loop(0, R // 8, surface, 0)
    part_ref[...] = mm3(fv[...], div_ref[:384, :], div_ref[384:, :]) + pick(surf_ref[...], sc_ref[...], 2)


def unpack(tiles, lane, t):
    value = roll(tiles[t], -3 * t)
    if t < 4:
        value = jnp.where(lane < 125 - 3 * t, value, roll(tiles[t + 1], -3 * (t + 1)))
    return value


def final_kernel(
    vtab_ref, ones_ref, own_ref, re_ref, ro_ref, rze_ref, rzo_ref, m_ref, part_ref, u_ref, pv_ref,
    res_ref, prod_ref, sums_ref,
    rcv, got, vx, vo, xs,
):
    join_received(rcv, re_ref, ro_ref)
    got[...] = own_ref[...] + choose(ones_ref[:, 256 : 256 + 2 * C], rcv[...], 2)
    even_z = parity("span")

    def gather(cb, carry):
        rows = cb * 8
        for l in range(L):
            scale = [m_ref[block(l * C + rows), a : a + 1] * HALF_LIFT for a in range(3)]
            for pt in range(2):
                at = block(pt * R + l * C + rows)
                values = [got[block(f * C + rows), tile_of(pt, l)] for f in range(4)]
                values += list(spanwise(vtab_ref, rze_ref, rzo_ref, even_z, rows, pt, l))
                for f, value in enumerate(values):
                    value = value * scale[f // 2]
                    vx[at, f * 128 : (f + 1) * 128] = value if f % 2 == 0 else -value
        return carry

    lax.fori_loop(0, C // 8, gather, 0)
    vo[...] = pick(vx[...], pv_ref[...], 2)
    lane = lanes()

    def output(rb, sums):
        sums = list(sums)
        rows = rb * 8
        prod = []
        for pt in range(2):
            tiles = [part_ref[block((pt * 5 + v) * R + rows), :] for v in range(5)]
            for v in range(4):
                tiles[v + 1] = tiles[v + 1] + vo[block(pt * R + rows), v * 128 : (v + 1) * 128]
            tiles = [jnp.where(lane < 125, x, 0.0) for x in tiles]
            for t in range(5):
                xs[block(pt * R + rows), t * 128 : (t + 1) * 128] = unpack(tiles, lane, t)
            prod.append(tiles)
        for v in range(5):
            d = u_ref[block((5 + v) * R + rows), :]
            res, p = prod[0][v], prod[1][v]
            for i, x in enumerate((d * p, d * d, res * res, p * p)):
                sums[i] = sums[i] + x
        return tuple(sums)

    zero = jnp.zeros((8, 128), F32)
    sums = lax.fori_loop(0, R // 8, output, (zero, zero, zero, zero))
    lane1 = lax.broadcasted_iota(jnp.int32, (1, 128), 1)
    row = jnp.zeros((1, 128), F32)
    for i, x in enumerate(sums):
        x = jnp.sum(jnp.sum(x, axis=0, keepdims=True), axis=1, keepdims=True)
        row = jnp.where(lane1 == i, x, row)
    sums_ref[...] = row
    for pt, ref in enumerate((res_ref, prod_ref)):
        for l in range(L):
            ref[:, l, :] = xs[pt * R + l * C : pt * R + (l + 1) * C, 0:625]


def scale_kernel(all_ref, prod_ref, dir_ref, basis_ref, krylov_ref, *, total):
    sums = jnp.sum(all_ref[...], axis=0, keepdims=True)
    dp, dd, rr, pp = [sums[:, i : i + 1] for i in range(4)]
    coefficient = dp / total
    beta = jnp.sqrt((pp - 2.0 * coefficient * dp + coefficient * coefficient * dd) / total)
    norm = jnp.sqrt(rr / total)
    for i, x in enumerate((coefficient, beta, norm)):
        krylov_ref[i] = x[0, 0]
    basis_ref[...] = (prod_ref[...] - coefficient.reshape(1, 1, 1) * dir_ref[...]) / beta.reshape(1, 1, 1)


def shaped(*dims):
    return jax.ShapeDtypeStruct(dims, F32)


def vmem(*dims):
    return pltpu.VMEM(dims, F32)


def pairs_of(count):
    first = [(i, i ^ 1) for i in range(count)]
    second = [(i, (((i + 1) ^ 1) - 1) % count) for i in range(count)]
    return first, second


def exchange(be, bo, ze, zo):
    se, so = pairs_of(lax.axis_size("stream"))
    pe, po = pairs_of(lax.axis_size("span"))
    return (
        lax.ppermute(be, "stream", se),
        lax.ppermute(bo, "stream", so),
        lax.ppermute(ze, "span", pe),
        lax.ppermute(zo, "span", po),
    )


SENT = (shaped(SLOTS, 512), shaped(SLOTS, 512), shaped(C, 256), shaped(C, 256))
VMEM_LIMIT = 20 * 2**20


def call(kernel, name, out_shape, scratch=(), **kwargs):
    params = pltpu.CompilerParams(vmem_limit_bytes=VMEM_LIMIT)
    return pl.pallas_call(kernel, out_shape=out_shape, scratch_shapes=list(scratch), name=name, compiler_params=params, **kwargs)


def local(state, direction, metric, face_source, send_rows):
    hbm = pl.BlockSpec(memory_space=pltpu.HBM)
    whole = pl.BlockSpec(memory_space=pltpu.VMEM)
    xs, tab, *sent = call(
        traces_kernel,
        "traces",
        (shaped(2 * R, 640), shaped(6 * C, 512)) + SENT,
        (vmem(C, L, 625), vmem(C, L, 625), pltpu.VMEM((640, 768), BF16), pltpu.SemaphoreType.DMA((3,))),
        in_specs=[hbm, hbm, hbm, whole],
    )(state, direction, CONST["trace"], send_rows)
    got = exchange(*sent)
    u, fl, w, q, m, ones, wall, own = call(
        before_kernel,
        "before",
        (
            shaped(10 * R, 128), shaped(10 * R, 256), shaped(8 * R, 128), shaped(8 * R, 384), shaped(R, 128),
            jax.ShapeDtypeStruct((4 * C, 384), BF16), shaped(4 * C, 128), shaped(4 * C, 512),
        ),
    )(xs, tab, jnp.transpose(metric, (2, 1, 0)), face_source.T, CONST["sel"], CONST["grad"])
    out, vv, vtab, *sent = call(
        gradient_kernel,
        "gradient",
        (shaped(10 * R, 256), shaped(2 * R, 1536), shaped(6 * C, 512)) + SENT,
        (vmem(2 * C, 512), vmem(4 * C, 512), vmem(8 * R, 256), vmem(8 * R, 384)),
    )(send_rows, tab, w, q, m, ones, wall, own, *got, CONST["lift_xy"], CONST["lift_z"], CONST["trace_v"])
    got = exchange(*sent)
    part, own = call(
        inner_kernel,
        "inner",
        (shaped(10 * R, 128), shaped(4 * C, 512)),
        (vmem(10 * R, 384), vmem(10 * R, 256)),
    )(u, fl, out, vv, vtab, ones, m, CONST["signs"], CONST["div"], CONST["scatter"])
    residual, product, sums = call(
        final_kernel,
        "final",
        (shaped(C, L, 625), shaped(C, L, 625), shaped(1, 128)),
        (vmem(2 * C, 512), vmem(4 * C, 512), vmem(2 * R, 768), vmem(2 * R, 512), vmem(2 * R, 640)),
    )(vtab, ones, own, *got, m, part, u, CONST["place_v"])
    axes = ("stream", "span")
    count = lax.axis_size("stream") * lax.axis_size("span")
    spread = jnp.broadcast_to(sums[None], (count, 1, 128))
    everyone = lax.all_to_all(spread, axes, 0, 0, tiled=True).reshape(count, 128)
    total = float(state.size * count)
    basis, krylov = call(
        lambda *refs: scale_kernel(*refs, total=total),
        "scale",
        (shaped(C, L, 625), shaped(3)),
        out_specs=(whole, pl.BlockSpec(memory_space=pltpu.SMEM)),
    )(everyone, product, direction)
    return residual, basis, krylov


def solution(mesh):
    cells = P("stream", "span", None)
    in_specs = (cells, cells, cells, P("stream", None), P("stream", None, None))
    out_specs = (cells, cells, P())
    return jax.shard_map(local, mesh=mesh, in_specs=in_specs, out_specs=out_specs, check_vma=False)
```
